32 devices in a mesh: vocab: 8 (over z, y), layer: 4 (over x, core).
Axes of the slice: x: 2, y: 2, z: 4, core: 2. Of those that a mesh axis runs over, the one named last changes fastest.
Arguments:
- residual: bfloat16 [1024, 8192], P('layer', 'vocab'), may hold values from -40 to 40
- gain: bfloat16 [1, 8192], P(None, 'vocab'), may hold values from 0.25 to 1.75
- unembed: bfloat16 [8192, 128256], P(None, ('vocab', 'layer')), may hold values from -0.22097087 to 0.22097087
Outputs:
- log_probs: float32 [1024, 128256], P('layer', 'vocab')
The draws below stay inside these ranges and needn't reach their ends.
All inputs are finite; a program needn't handle non-finite values.
Results may differ from the reference program's by a relative error of at most 0.0003.
Values may be sent and summed in bfloat16 or wider, within the bound.
No kernel may reach another device: no remote copies, remote signals or barrier semaphores. Data moves between devices by JAX's collectives and lax.ppermute only.
A program may use at most 192 MiB of HBM per device.

```python
import math
import jax
import jax.numpy as jnp
from jax import lax

D = 8192
VOCAB = 128256
TOK = 16
ROWS = 1024


def loud_offset(key):
    return jax.random.randint(jax.random.fold_in(key, 103), (), 0, 32)


def column_of(key, column):
    gaussian = jax.random.truncated_normal(jax.random.fold_in(jax.random.fold_in(key, 101), column), -4.0, 4.0, (D,), jnp.float32)
    spread = jax.random.uniform(jax.random.fold_in(jax.random.fold_in(key, 102), column), (), jnp.float32, -0.5, 0.5)
    loud = jnp.where(column % 32 == loud_offset(key), max(1.0, 80.0 / math.sqrt(D)), 1.0)
    return gaussian * (3.0 * jnp.exp(spread) * loud / math.sqrt(D))


def unit_column(key, column):
    vector = column_of(key, column)
    return vector / jnp.sqrt(jnp.mean(vector * vector))


def draw_unembed(key, part):
    columns = jax.vmap(lambda column: column_of(key, column))(jnp.arange(VOCAB))
    return columns.T.astype(jnp.bfloat16)


def draw_residual(key, part):
    offset = loud_offset(key)
    first = offset + 32 * jax.random.randint(jax.random.fold_in(key, 203), (ROWS,), 0, VOCAB // 32)
    second = offset + 32 * jax.random.randint(jax.random.fold_in(key, 204), (ROWS,), 0, VOCAB // 32)
    aligned = jax.vmap(lambda column: unit_column(key, column))(first)
    aligned = aligned + 0.99 * jax.vmap(lambda column: unit_column(key, column))(second)
    chosen = (jnp.arange(ROWS) % TOK == 0)[:, None]
    noise = jax.random.truncated_normal(jax.random.fold_in(key, 201), -4.0, 4.0, (ROWS, D), jnp.float32)
    scales = jnp.exp(jax.random.uniform(jax.random.fold_in(key, 202), (ROWS, 1), jnp.float32, 0.0, math.log(10.0)))
    strength = jnp.exp(jax.random.uniform(jax.random.fold_in(key, 205), (ROWS, 1), jnp.float32, math.log(0.2), math.log(2.0)))
    mixed = jnp.where(chosen, strength * (aligned + 0.1 * noise), noise * scales)
    return mixed.astype(jnp.bfloat16)


def setup_inputs(seed: int = 0) -> dict:
    key_of = jax.random.split(jax.random.key(seed), 4)
    residual = draw_residual(jax.random.fold_in(key_of[3], 71), 0)
    gain = jnp.clip(1.0 + 0.15 * jax.random.normal(key_of[1], (1, D), jnp.float32), 0.25, 1.75).astype(jnp.bfloat16)
    unembed = draw_unembed(jax.random.fold_in(key_of[3], 71), 0)
    return dict(residual=residual, gain=gain, unembed=unembed)


def reference(residual, gain, unembed):
    widened = residual.astype(jnp.float32)
    inverse = lax.rsqrt(lax.optimization_barrier(jnp.sum(widened * widened, axis=1)) / D + 1e-05)
    scaled = (widened * gain.astype(jnp.float32)).astype(jnp.bfloat16)
    logits = jnp.dot(scaled, unembed, preferred_element_type=jnp.float32) * inverse[:, None]
    highest = lax.optimization_barrier(jnp.max(logits, axis=1, keepdims=True))
    lse = highest + jnp.log(lax.optimization_barrier(jnp.sum(jnp.exp(logits - highest), axis=1, keepdims=True)))
    return logits - lse
```

```python
import functools

import jax
import jax.numpy as jnp
from jax import lax
from jax.experimental import pallas as pl
from jax.experimental.pallas import tpu as pltpu
from jax.sharding import PartitionSpec as P


EPS = 1e-05
TILE = 512
CHUNK = 1024
FIRST, LATER = 1024, 1536
DEPTH = 4
SPAN = 250.0
LN2 = 0.6931471805599453
AXES = ("vocab", "layer")
F32 = jnp.float32
BF16 = jnp.bfloat16
VMEM_LIMIT = 28 * 1024 * 1024
JOIN_LIMIT = 12 * 1024 * 1024
NT = (((1,), (1,)), ((), ()))
HBM = pl.BlockSpec(memory_space=pl.ANY)
VMEM = pl.BlockSpec(memory_space=pltpu.VMEM)


def sum_slots(rows, width):
    piece = min(rows, width)
    per_tile = width // piece
    slots = []
    for q in range(3 * (rows // piece)):
        slots.append((q // (rows // piece), (q % (rows // piece)) * piece, 16 * (q // per_tile), (q % per_tile) * piece))
    return piece, slots, 16 * (slots[-1][2] // 16 + 1)


def pack_kernel(residual_ref, gain_ref, out_ref):
    rows, width = residual_ref.shape
    piece, slots, _ = sum_slots(rows, width)
    wide = residual_ref[...].astype(F32)
    out_ref[pl.ds(0, rows), :] = (wide * gain_ref[...].astype(F32)).astype(BF16)
    square = wide * wide
    high = square.astype(BF16)
    low = (square - high.astype(F32)).astype(BF16)
    ones = jnp.ones((16, width), BF16)
    sums = lax.dot_general(ones, high, NT, preferred_element_type=F32)
    sums = sums + lax.dot_general(ones, low, NT, preferred_element_type=F32)
    parts = []
    for _ in range(3):
        part = sums.astype(BF16)
        sums = sums - part.astype(F32)
        parts.append(part)
    out_ref[pl.ds(rows, out_ref.shape[0] - rows), :] = jnp.zeros((out_ref.shape[0] - rows, width), BF16)
    for part, first, row, lane in slots:
        out_ref[pl.ds(rows + row, 16), pl.ds(lane, piece)] = parts[part][:, first : first + piece]


def pack(residual, gain):
    rows, width = residual.shape
    extra = sum_slots(rows, width)[2]
    return pl.pallas_call(
        pack_kernel,
        out_shape=jax.ShapeDtypeStruct((rows + extra, width), BF16),
        in_specs=[VMEM, VMEM],
        out_specs=VMEM,
    )(residual, gain)


def join_kernel(n_groups, stacks, indices, rows, *refs):
    n = len(stacks)
    block_refs = refs[: n * n_groups]
    a_ref, inverse_ref, sums_ref, sem = refs[n * n_groups + 1 :]
    width = block_refs[0].shape[2]
    piece, slots, extra = sum_slots(rows, width)
    vocab = lax.axis_index("vocab")
    copies = []
    for g in range(n_groups):
        slot = 0
        for j in range(n):
            ref = block_refs[g * n + j]
            for k in range(stacks[j]):
                at = pl.multiple_of(indices[j](vocab, k) * width, width)
                copies.append(pltpu.make_async_copy(ref.at[k, pl.ds(0, rows), :], a_ref.at[pl.ds(g * rows, rows), pl.ds(at, width)], sem))
                copies.append(pltpu.make_async_copy(ref.at[k, pl.ds(rows, extra), :], sums_ref.at[g, slot], sem))
                slot += 1
    for copy in copies:
        copy.start()
    for copy in copies:
        copy.wait()
    for g in range(n_groups):
        for row_first in range(0, rows, piece):
            total = jnp.zeros((16, piece), F32)
            for part, at, row, lane in slots:
                if at == row_first:
                    total = total + jnp.sum(sums_ref[g, :, pl.ds(row, 16), pl.ds(lane, piece)].astype(F32), axis=0)
            features = width * sum(stacks)
            inverse = lax.rsqrt(total / features + EPS)
            inverse_ref[:, pl.ds(g * rows + row_first, piece)] = inverse[0:8, :]


def join(groups, indices, rows, after):
    stacks = [block.shape[0] for block in groups[0]]
    width = groups[0][0].shape[2]
    extra, features = sum_slots(rows, width)[2], width * sum(stacks)
    total = rows * len(groups)
    return pl.pallas_call(
        functools.partial(join_kernel, len(groups), stacks, indices, rows),
        out_shape=[jax.ShapeDtypeStruct((total, features), BF16), jax.ShapeDtypeStruct((8, total), F32)],
        in_specs=[HBM] * (len(stacks) * len(groups) + 1),
        out_specs=[VMEM, VMEM],
        scratch_shapes=[pltpu.VMEM((len(groups), sum(stacks), extra, width), BF16), pltpu.SemaphoreType.DMA],
        compiler_params=pltpu.CompilerParams(vmem_limit_bytes=JOIN_LIMIT),
        cost_estimate=pl.CostEstimate(flops=total * features, bytes_accessed=4 * total * features, transcendentals=0),
    )(*[block for group in groups for block in group], after)


def logits_kernel(n_groups, rows, columns, first, partial, w_ref, a_ref, inverse_ref, after_ref, *outs):
    del after_ref
    code_refs, stat_refs = outs[:n_groups], outs[n_groups:]
    step = pl.program_id(0)
    products = lax.dot_general(w_ref[...], a_ref[...], NT, preferred_element_type=F32)
    logits = products * inverse_ref[0:1, :]
    if partial:
        entry = first + step * TILE + lax.broadcasted_iota(jnp.int32, logits.shape, 0)
        valid = entry < columns
        logits = jnp.where(valid, logits, logits[0:1, :])
    high = jnp.max(logits, axis=0, keepdims=True)
    low = jnp.min(logits, axis=0, keepdims=True)
    scale = SPAN / jnp.maximum(high - low, 1e-6)
    codes = jnp.exp2((logits - (high + low) * 0.5) * scale).astype(BF16)
    powers = jnp.exp(logits - high)
    if partial:
        powers = jnp.where(valid, powers, 0.0)
    total = jnp.sum(powers, axis=0, keepdims=True)
    stats = jnp.concatenate([high, low, total] + [jnp.zeros_like(high)] * 5, axis=0)
    for g in range(n_groups):
        code_refs[g][...] = codes[:, g * rows : (g + 1) * rows]
        stat_refs[g][...] = stats[:, g * rows : (g + 1) * rows]


def logits_call(weights, joined, after, rows, first, count):
    scaled, inverse = joined
    columns, features = weights.shape
    n_groups, tiles = scaled.shape[0] // rows, pl.cdiv(count, TILE)
    base = first // TILE
    out = pl.pallas_call(
        functools.partial(logits_kernel, n_groups, rows, columns, first, count % TILE != 0),
        grid=(tiles,),
        in_specs=[pl.BlockSpec((TILE, features), lambda i: (base + i, 0)), VMEM, VMEM, HBM],
        out_specs=[pl.BlockSpec((TILE, rows), lambda i: (i, 0))] * n_groups + [pl.BlockSpec((8, rows), lambda i: (i, 0))] * n_groups,
        out_shape=[jax.ShapeDtypeStruct((count, rows), BF16)] * n_groups + [jax.ShapeDtypeStruct((8 * tiles, rows), F32)] * n_groups,
        compiler_params=pltpu.CompilerParams(vmem_limit_bytes=VMEM_LIMIT),
        cost_estimate=pl.CostEstimate(
            flops=2 * count * features * rows * n_groups,
            bytes_accessed=2 * count * features + 2 * rows * n_groups * features,
            transcendentals=2 * count * rows * n_groups,
        ),
    )(weights, scaled, inverse, after)
    return out[:n_groups], out[n_groups:]


def combine_kernel(*refs):
    *stat_refs, out_ref = refs
    tiles = [ref[pl.ds(8 * i, 8), :] for ref in stat_refs for i in range(ref.shape[0] // 8)]
    highest = functools.reduce(jnp.maximum, [tile[0:1, :] for tile in tiles])
    total = sum(tile[2:3, :] * jnp.exp(tile[0:1, :] - highest) for tile in tiles)
    out_ref[...] = jnp.concatenate([highest, highest, total] + [jnp.zeros_like(total)] * 5, axis=0)


def combine(stats):
    return pl.pallas_call(
        combine_kernel,
        out_shape=jax.ShapeDtypeStruct((8, stats[0].shape[1]), F32),
        in_specs=[VMEM] * len(stats),
        out_specs=VMEM,
    )(*stats)


def row_lse(totals_refs):
    pairs = [ref[pl.ds(8 * i, 8), :] for ref in totals_refs for i in range(ref.shape[0] // 8)]
    highest = functools.reduce(jnp.maximum, [pair[0:1, :] for pair in pairs])
    total = sum(pair[2:3, :] * jnp.exp(pair[0:1, :] - highest) for pair in pairs)
    return highest + jnp.log(total)


def decode_terms(stats, tile, lse):
    high, low = stats[8 * tile : 8 * tile + 1, :], stats[8 * tile + 1 : 8 * tile + 2, :]
    factor = jnp.maximum(high - low, 1e-6) * (1.0 / (SPAN * LN2))
    return factor, (high + low) * 0.5 - lse


def write_kernel(items, n_stats, n_totals, has_previous, columns, *refs):
    n_codes = 1 + max(item[4] for item in items)
    code_refs = refs[:n_codes]
    stat_refs = refs[n_codes : n_codes + n_stats]
    totals_refs = refs[n_codes + n_stats : n_codes + n_stats + n_totals]
    rest = refs[n_codes + n_stats + n_totals + has_previous :]
    out_ref, in_buf, out_buf, in_sem, out_sem = rest
    lse = row_lse(totals_refs)
    layer = lax.axis_index("layer")
    depth = DEPTH

    def fetch(i):
        count, ref, at = items[i][0], items[i][4], items[i][5]
        return pltpu.make_async_copy(code_refs[ref].at[pl.ds(at, count), :], in_buf.at[i % depth, pl.ds(0, count), :], in_sem.at[i % depth])

    def put(i):
        count, first, distance = items[i][:3]
        at = pl.multiple_of((layer ^ distance) * columns + first, 8)
        return pltpu.make_async_copy(out_buf.at[i % depth, pl.ds(0, count), :], out_ref.at[pl.ds(at, count), :], out_sem.at[i % depth])

    for i in range(min(depth, len(items))):
        fetch(i).start()
    for i, (count, first, distance, source, _, _) in enumerate(items):
        fetch(i).wait()
        if i >= depth:
            put(i - depth).wait()
        for at in range(0, count, TILE):
            size = min(TILE, count - at)
            factor, shift = decode_terms(stat_refs[source], (first + at) // TILE, lse)
            codes = in_buf[i % depth, pl.ds(at, size), :].astype(F32)
            out_buf[i % depth, pl.ds(at, size), :] = jnp.log(codes) * factor + shift
        put(i).start()
        if i + depth < len(items):
            fetch(i + depth).start()
    for i in range(max(0, len(items) - depth), len(items)):
        put(i).wait()


def write(codes, items, stats, totals, previous, columns, out_rows):
    rows = codes[0].shape[1]
    size = max(item[0] for item in items)
    n_in = len(codes) + len(stats) + len(totals)
    return pl.pallas_call(
        functools.partial(write_kernel, items, len(stats), len(totals), int(previous is not None), columns),
        out_shape=jax.ShapeDtypeStruct((out_rows, rows), F32),
        in_specs=[HBM] * len(codes) + [VMEM] * (len(stats) + len(totals)) + [HBM] * int(previous is not None),
        out_specs=HBM,
        scratch_shapes=[
            pltpu.VMEM((DEPTH, size, rows), BF16),
            pltpu.VMEM((DEPTH, size, rows), F32),
            pltpu.SemaphoreType.DMA((DEPTH,)),
            pltpu.SemaphoreType.DMA((DEPTH,)),
        ],
        input_output_aliases={n_in: 0} if previous is not None else {},
        cost_estimate=pl.CostEstimate(flops=0, bytes_accessed=6 * rows * sum(item[0] for item in items), transcendentals=0),
    )(*codes, *stats, *totals, *([previous] if previous is not None else []))


def chunks_of(columns):
    edges = [0] + list(range(FIRST, columns, LATER)) + [columns]
    return [(first, last - first) for first, last in zip(edges, edges[1:])]


def local(n_vocab, n_layer, residual, gain, unembed):
    rows = residual.shape[0]
    weights = unembed.T
    columns = weights.shape[0]

    def permute(x, move):
        pairs = []
        for v in range(n_vocab):
            for l in range(n_layer):
                to_v, to_l = move(v, l)
                pairs.append((v * n_layer + l, to_v * n_layer + to_l))
        return lax.ppermute(x, AXES, pairs)

    def over_layer(x, distance):
        return permute(x, lambda v, l: (v, l ^ distance))

    n_far = n_vocab // 2
    direct = n_far <= 4

    def over_vocab(x, far, flip):
        return permute(x, lambda v, l: (((v // 2 + far) % n_far) * 2 + ((v % 2) ^ flip), l))

    far_steps = sorted(range(1, n_far), key=lambda o: min(o, n_far - o))

    steps = [0] + far_steps

    def gather(block, given={}):
        if not direct:
            return {0: lax.all_gather(block, "vocab")}
        blocks = {("z", 0): block, **given}
        for o in far_steps:
            if ("z", o) not in blocks:
                blocks["z", o] = over_vocab(block, o, 0)
        for o in steps:
            if ("y", o) not in blocks:
                blocks["y", o] = over_vocab(blocks["z", o], 0, 1)
        return {key: blocks[key] for axis in "zy" for o in steps for key in [(axis, o)]}

    shared = [("z", far_steps[0]), ("y", 0)] if direct else []

    if direct:
        indices = [
            functools.partial(lambda o, flip, vocab, k: lax.rem(vocab // 2 + n_far - o, n_far) * 2 + lax.rem(vocab + flip, 2), o, flip)
            for flip in (0, 1)
            for o in steps
        ]
    else:
        indices = [lambda vocab, k: k]

    payload = pack(residual, gain)
    evens = sorted(range(0, n_layer, 2), reverse=True)
    remote = {}
    own = gather(payload)
    for e in evens[:-1]:
        given = {key: over_layer(own[key], e) for key in shared}
        remote[e] = gather(over_layer(payload, e), given)

    chunks = chunks_of(columns)
    codes, stats = {d: [] for d in range(n_layer)}, {d: [] for d in range(n_layer)}
    after = payload
    for e in evens:
        mine = own if e == 0 else remote[e]
        theirs = {key: over_layer(x, 1) for key, x in mine.items()}
        groups = [[x if x.ndim == 3 else x[None] for x in part.values()] for part in (mine, theirs)]
        joined = join(groups, indices, rows, after)
        for first, count in chunks if e else [(0, columns)]:
            new_codes, new_stats = logits_call(weights, joined, after, rows, first, count)
            after = new_stats[0]
            for d in (e, e + 1):
                code = new_codes[d - e]
                codes[d].append(over_layer(code, d) if d else code)
                stats[d].append(new_stats[d - e])
    for d in range(n_layer):
        stat = stats[d][0] if len(stats[d]) == 1 else jnp.concatenate(stats[d])
        stats[d] = over_layer(stat, d) if d else stat

    distances = [0, 1] + [d for e in evens[:-1] for d in (e, e + 1)]
    total = combine([stats[d] for d in distances])
    if direct:
        total = combine([total, over_vocab(total, 0, 1)])
        totals = [total] + [over_vocab(total, o, 0) for o in far_steps]
    else:
        totals = [lax.all_gather(total, "vocab", tiled=True)]

    if columns % 8:
        lse = row_lse([jnp.concatenate(totals)])
        pieces = []
        for d in range(n_layer):
            code, parts = jnp.concatenate(codes[d]), []
            for at in range(0, columns, TILE):
                factor, shift = decode_terms(stats[d], at // TILE, lse)
                parts.append(jnp.log(code[at : at + TILE].astype(F32)) * factor + shift)
            pieces.append(jnp.concatenate(parts))
        order = lax.axis_index("layer") ^ jnp.arange(n_layer)
        return jnp.take(jnp.stack(pieces), order, axis=0).reshape(n_layer * columns, rows).T

    early, late = [], []
    for d in distances:
        first = 0
        for array in codes[d]:
            for at in range(0, array.shape[0], CHUNK):
                early.append((array, (min(CHUNK, array.shape[0] - at), first + at, d, distances.index(d), at)))
            first += array.shape[0]
    early, late = early[:-1], early[-1:]
    out = None
    for part in (early, late):
        arrays, items = [], []
        for array, (count, first, d, source, at) in part:
            if not any(array is seen for seen in arrays):
                arrays.append(array)
            ref = [array is seen for seen in arrays].index(True)
            items.append((count, first, d, source, ref, at))
        out = write(arrays, items, [stats[d] for d in distances], totals, out, columns, n_layer * columns)
    return out.T


def solution(mesh):
    placed = (P("layer", "vocab"), P(None, "vocab"), P(None, ("vocab", "layer")))
    n_vocab, n_layer = mesh.shape["vocab"], mesh.shape["layer"]

    def body(residual, gain, unembed):
        return local(n_vocab, n_layer, residual, gain, unembed)

    mapped = jax.shard_map(body, mesh=mesh, in_specs=placed, out_specs=P("layer", "vocab"), check_vma=False)

    def step(residual, gain, unembed):
        return mapped(residual, gain, unembed)

    return step if n_vocab // 2 <= 4 else mapped
```

```python
import functools

import jax
import jax.numpy as jnp
from jax import lax
from jax.experimental import pallas as pl
from jax.experimental.pallas import tpu as pltpu
from jax.sharding import PartitionSpec as P


EPS = 1e-05
TILE = 512
CHUNK = 1024
EDGES = (1536,)
AHEAD = 0
DEPTH = 4
SPAN = 250.0
LN2 = 0.6931471805599453
AXES = ("vocab", "layer")
F32 = jnp.float32
BF16 = jnp.bfloat16
VMEM_LIMIT, SPLIT_LIMIT, PART_LIMIT = 28 * 1024 * 1024, 20 * 1024 * 1024, 14 * 1024 * 1024
JOIN_LIMIT = 12 * 1024 * 1024
NT = (((1,), (1,)), ((), ()))
HBM = pl.BlockSpec(memory_space=pl.ANY)
VMEM = pl.BlockSpec(memory_space=pltpu.VMEM)


def sum_slots(rows, width):
    piece = min(rows, width)
    per_tile = width // piece
    slots = []
    for q in range(3 * (rows // piece)):
        slots.append((q // (rows // piece), (q % (rows // piece)) * piece, 16 * (q // per_tile), (q % per_tile) * piece))
    return piece, slots, 16 * (slots[-1][2] // 16 + 1)


def pack_kernel(residual_ref, gain_ref, out_ref):
    rows, width = residual_ref.shape
    piece, slots, _ = sum_slots(rows, width)
    wide = residual_ref[...].astype(F32)
    out_ref[pl.ds(0, rows), :] = (wide * gain_ref[...].astype(F32)).astype(BF16)
    square = wide * wide
    high = square.astype(BF16)
    low = (square - high.astype(F32)).astype(BF16)
    ones = jnp.ones((16, width), BF16)
    sums = lax.dot_general(ones, high, NT, preferred_element_type=F32)
    sums = sums + lax.dot_general(ones, low, NT, preferred_element_type=F32)
    parts = []
    for _ in range(3):
        part = sums.astype(BF16)
        sums = sums - part.astype(F32)
        parts.append(part)
    out_ref[pl.ds(rows, out_ref.shape[0] - rows), :] = jnp.zeros((out_ref.shape[0] - rows, width), BF16)
    for part, first, row, lane in slots:
        out_ref[pl.ds(rows + row, 16), pl.ds(lane, piece)] = parts[part][:, first : first + piece]


def pack(residual, gain):
    rows, width = residual.shape
    extra = sum_slots(rows, width)[2]
    return pl.pallas_call(
        pack_kernel,
        out_shape=jax.ShapeDtypeStruct((rows + extra, width), BF16),
        in_specs=[VMEM, VMEM],
        out_specs=VMEM,
    )(residual, gain)


def join_kernel(n_groups, all_features, stacks, indices, rows, *refs):
    n = len(stacks)
    block_refs = refs[: n * n_groups]
    before_ref = refs[n * n_groups + 1]
    a_ref, total_ref, inverse_ref, sums_ref, sem = refs[n * n_groups + 2 :]
    width = block_refs[0].shape[2]
    piece, slots, extra = sum_slots(rows, width)
    vocab = lax.axis_index("vocab")
    copies = []
    for g in range(n_groups):
        slot = 0
        for j in range(n):
            ref = block_refs[g * n + j]
            for k in range(stacks[j]):
                at = slot * width if indices is None else pl.multiple_of(indices[j](vocab, k) * width, width)
                copies.append(pltpu.make_async_copy(ref.at[k, pl.ds(0, rows), :], a_ref.at[pl.ds(g * rows, rows), pl.ds(at, width)], sem))
                copies.append(pltpu.make_async_copy(ref.at[k, pl.ds(rows, extra), :], sums_ref.at[g, slot], sem))
                slot += 1
    for copy in copies:
        copy.start()
    for copy in copies:
        copy.wait()
    for g in range(n_groups):
        for row_first in range(0, rows, piece):
            total = jnp.zeros((16, piece), F32)
            for part, at, row, lane in slots:
                if at == row_first:
                    total = total + jnp.sum(sums_ref[g, :, pl.ds(row, 16), pl.ds(lane, piece)].astype(F32), axis=0)
            lanes = pl.ds(g * rows + row_first, piece)
            total = total[0:8, :] + before_ref[:, lanes]
            total_ref[:, lanes] = total
            inverse_ref[:, lanes] = lax.rsqrt(total / all_features + EPS)


def join(groups, all_features, indices, rows, after, before):
    stacks = [block.shape[0] for block in groups[0]]
    width = groups[0][0].shape[2]
    extra, features = sum_slots(rows, width)[2], width * sum(stacks)
    total = rows * len(groups)
    if before is None:
        before = jnp.zeros((8, total), F32)
    return pl.pallas_call(
        functools.partial(join_kernel, len(groups), all_features, stacks, indices, rows),
        out_shape=[jax.ShapeDtypeStruct((total, features), BF16)] + [jax.ShapeDtypeStruct((8, total), F32)] * 2,
        in_specs=[HBM] * (len(stacks) * len(groups) + 1) + [VMEM],
        out_specs=[VMEM] * 3,
        scratch_shapes=[pltpu.VMEM((len(groups), sum(stacks), extra, width), BF16), pltpu.SemaphoreType.DMA],
        compiler_params=pltpu.CompilerParams(vmem_limit_bytes=JOIN_LIMIT),
        cost_estimate=pl.CostEstimate(flops=total * features, bytes_accessed=4 * total * features, transcendentals=0),
    )(*[block for group in groups for block in group], after, before)


def multiply(w_refs, a_ref):
    width = w_refs[0].shape[1]
    terms = [
        lax.dot_general(w_ref[...], a_ref[:, i * width : (i + 1) * width], NT, preferred_element_type=F32)
        for i, w_ref in enumerate(w_refs)
    ]
    return functools.reduce(jnp.add, terms)


def part_kernel(n_blocks, place_ref, *refs):
    del place_ref
    refs[-1][...] = multiply(refs[:n_blocks], refs[n_blocks])


def weight_specs(base, places, features):
    if places is None:
        return [pl.BlockSpec((TILE, features), lambda i, place: (base + i, 0))]
    width = features // places.shape[0]
    return [pl.BlockSpec((TILE, width), lambda i, place, j=j: (base + i, place[j])) for j in range(places.shape[0])]


def part_call(weights, scaled, places, after, first, count):
    rows, features = scaled.shape
    specs = weight_specs(first // TILE, places, features)
    return pl.pallas_call(
        functools.partial(part_kernel, len(specs)),
        grid_spec=pltpu.PrefetchScalarGridSpec(
            num_scalar_prefetch=1,
            grid=(pl.cdiv(count, TILE),),
            in_specs=specs + [VMEM, HBM],
            out_specs=pl.BlockSpec((TILE, rows), lambda i, place: (i, 0)),
        ),
        out_shape=jax.ShapeDtypeStruct((count, rows), F32),
        compiler_params=pltpu.CompilerParams(vmem_limit_bytes=PART_LIMIT),
        cost_estimate=pl.CostEstimate(
            flops=2 * count * features * rows, bytes_accessed=2 * count * features + 4 * rows * count, transcendentals=0
        ),
    )(places, *[weights] * len(specs), scaled, after)


def logits_kernel(n_blocks, n_groups, rows, columns, first, partial, has_part, place_ref, *refs):
    del place_ref
    a_ref, inverse_ref = refs[n_blocks : n_blocks + 2]
    outs = refs[n_blocks + 3 + has_part :]
    code_refs, stat_refs = outs[:n_groups], outs[n_groups:]
    step = pl.program_id(0)
    products = multiply(refs[:n_blocks], a_ref)
    if has_part:
        products = products + refs[n_blocks + 3][...]
    logits = products * inverse_ref[0:1, :]
    if partial:
        entry = first + step * TILE + lax.broadcasted_iota(jnp.int32, logits.shape, 0)
        valid = entry < columns
        logits = jnp.where(valid, logits, logits[0:1, :])
    high = jnp.max(logits, axis=0, keepdims=True)
    low = jnp.min(logits, axis=0, keepdims=True)
    scale = SPAN / jnp.maximum(high - low, 1e-6)
    codes = jnp.exp2((logits - (high + low) * 0.5) * scale).astype(BF16)
    powers = jnp.exp(logits - high)
    if partial:
        powers = jnp.where(valid, powers, 0.0)
    total = jnp.sum(powers, axis=0, keepdims=True)
    stats = jnp.concatenate([high, low, total] + [jnp.zeros_like(high)] * 5, axis=0)
    for g in range(n_groups):
        code_refs[g][...] = codes[:, g * rows : (g + 1) * rows]
        stat_refs[g][...] = stats[:, g * rows : (g + 1) * rows]


def logits_call(weights, joined, places, part, after, rows, first, count):
    scaled, _, inverse = joined
    columns, features = weights.shape[0], scaled.shape[1]
    n_groups, tiles = scaled.shape[0] // rows, pl.cdiv(count, TILE)
    specs = weight_specs(first // TILE, places, features)
    if places is None:
        places = jnp.zeros((1,), jnp.int32)
    n_blocks, has_part = len(specs), int(part is not None)
    specs = specs + [VMEM, VMEM, HBM] + [pl.BlockSpec((TILE, scaled.shape[0]), lambda i, place: (i, 0))] * has_part
    out = pl.pallas_call(
        functools.partial(logits_kernel, n_blocks, n_groups, rows, columns, first, count % TILE != 0, has_part),
        grid_spec=pltpu.PrefetchScalarGridSpec(
            num_scalar_prefetch=1,
            grid=(tiles,),
            in_specs=specs,
            out_specs=[pl.BlockSpec((TILE, rows), lambda i, place: (i, 0))] * n_groups
            + [pl.BlockSpec((8, rows), lambda i, place: (i, 0))] * n_groups,
        ),
        out_shape=[jax.ShapeDtypeStruct((count, rows), BF16)] * n_groups + [jax.ShapeDtypeStruct((8 * tiles, rows), F32)] * n_groups,
        compiler_params=pltpu.CompilerParams(vmem_limit_bytes=SPLIT_LIMIT if has_part else VMEM_LIMIT),
        cost_estimate=pl.CostEstimate(
            flops=2 * count * features * rows * n_groups,
            bytes_accessed=2 * count * features + 2 * rows * n_groups * features,
            transcendentals=2 * count * rows * n_groups,
        ),
    )(places, *[weights] * n_blocks, scaled, inverse, after, *([part] if has_part else []))
    return out[:n_groups], out[n_groups:]


def combine_kernel(*refs):
    *stat_refs, out_ref = refs
    tiles = [ref[pl.ds(8 * i, 8), :] for ref in stat_refs for i in range(ref.shape[0] // 8)]
    highest = functools.reduce(jnp.maximum, [tile[0:1, :] for tile in tiles])
    total = sum(tile[2:3, :] * jnp.exp(tile[0:1, :] - highest) for tile in tiles)
    out_ref[...] = jnp.concatenate([highest, highest, total] + [jnp.zeros_like(total)] * 5, axis=0)


def combine(stats):
    return pl.pallas_call(
        combine_kernel,
        out_shape=jax.ShapeDtypeStruct((8, stats[0].shape[1]), F32),
        in_specs=[VMEM] * len(stats),
        out_specs=VMEM,
    )(*stats)


def row_lse(totals_refs):
    pairs = [ref[pl.ds(8 * i, 8), :] for ref in totals_refs for i in range(ref.shape[0] // 8)]
    highest = functools.reduce(jnp.maximum, [pair[0:1, :] for pair in pairs])
    total = sum(pair[2:3, :] * jnp.exp(pair[0:1, :] - highest) for pair in pairs)
    return highest + jnp.log(total)


def decode_terms(stats, tile, lse):
    high, low = stats[8 * tile : 8 * tile + 1, :], stats[8 * tile + 1 : 8 * tile + 2, :]
    factor = jnp.maximum(high - low, 1e-6) * (1.0 / (SPAN * LN2))
    return factor, (high + low) * 0.5 - lse


def write_kernel(items, n_stats, n_totals, has_previous, columns, *refs):
    n_codes = 1 + max(item[4] for item in items)
    code_refs = refs[:n_codes]
    stat_refs = refs[n_codes : n_codes + n_stats]
    totals_refs = refs[n_codes + n_stats : n_codes + n_stats + n_totals]
    rest = refs[n_codes + n_stats + n_totals + has_previous :]
    out_ref, in_buf, out_buf, in_sem, out_sem = rest
    lse = row_lse(totals_refs)
    layer = lax.axis_index("layer")
    depth = DEPTH

    def fetch(i):
        count, ref, at = items[i][0], items[i][4], items[i][5]
        return pltpu.make_async_copy(code_refs[ref].at[pl.ds(at, count), :], in_buf.at[i % depth, pl.ds(0, count), :], in_sem.at[i % depth])

    def put(i):
        count, first, distance = items[i][:3]
        at = pl.multiple_of((layer ^ distance) * columns + first, 8)
        return pltpu.make_async_copy(out_buf.at[i % depth, pl.ds(0, count), :], out_ref.at[pl.ds(at, count), :], out_sem.at[i % depth])

    for i in range(min(depth, len(items))):
        fetch(i).start()
    for i, (count, first, distance, source, _, _) in enumerate(items):
        fetch(i).wait()
        if i >= depth:
            put(i - depth).wait()
        for at in range(0, count, TILE):
            size = min(TILE, count - at)
            factor, shift = decode_terms(stat_refs[source], (first + at) // TILE, lse)
            codes = in_buf[i % depth, pl.ds(at, size), :].astype(F32)
            out_buf[i % depth, pl.ds(at, size), :] = jnp.log(codes) * factor + shift
        put(i).start()
        if i + depth < len(items):
            fetch(i + depth).start()
    for i in range(max(0, len(items) - depth), len(items)):
        put(i).wait()


def write(codes, items, stats, totals, previous, columns, out_rows):
    rows = codes[0].shape[1]
    size = max(item[0] for item in items)
    n_in = len(codes) + len(stats) + len(totals)
    return pl.pallas_call(
        functools.partial(write_kernel, items, len(stats), len(totals), int(previous is not None), columns),
        out_shape=jax.ShapeDtypeStruct((out_rows, rows), F32),
        in_specs=[HBM] * len(codes) + [VMEM] * (len(stats) + len(totals)) + [HBM] * int(previous is not None),
        out_specs=HBM,
        scratch_shapes=[
            pltpu.VMEM((DEPTH, size, rows), BF16),
            pltpu.VMEM((DEPTH, size, rows), F32),
            pltpu.SemaphoreType.DMA((DEPTH,)),
            pltpu.SemaphoreType.DMA((DEPTH,)),
        ],
        input_output_aliases={n_in: 0} if previous is not None else {},
        cost_estimate=pl.CostEstimate(flops=0, bytes_accessed=6 * rows * sum(item[0] for item in items), transcendentals=0),
    )(*codes, *stats, *totals, *([previous] if previous is not None else []))


def chunks_of(columns):
    edges = [0] + [edge for edge in EDGES if edge < columns] + [columns]
    return [(first, last - first) for first, last in zip(edges, edges[1:])]


def local(n_vocab, n_layer, residual, gain, unembed):
    rows = residual.shape[0]
    weights = unembed.T
    columns, features = weights.shape

    def permute(x, move):
        pairs = []
        for v in range(n_vocab):
            for l in range(n_layer):
                to_v, to_l = move(v, l)
                pairs.append((v * n_layer + l, to_v * n_layer + to_l))
        return lax.ppermute(x, AXES, pairs)

    def over_layer(x, distance):
        return permute(x, lambda v, l: (v, l ^ distance))

    n_far = n_vocab // 2
    direct = n_far <= 4

    def over_vocab(x, far, flip):
        return permute(x, lambda v, l: (((v // 2 + far) % n_far) * 2 + ((v % 2) ^ flip), l))

    far_steps = sorted(range(1, n_far), key=lambda o: min(o, n_far - o))

    steps = [0] + far_steps

    def gather(block, given={}):
        if not direct:
            return {0: lax.all_gather(block, "vocab")}
        blocks = {("z", 0): block, **given}
        for o in far_steps:
            if ("z", o) not in blocks:
                blocks["z", o] = over_vocab(block, o, 0)
        for o in steps:
            if ("y", o) not in blocks:
                blocks["y", o] = over_vocab(blocks["z", o], 0, 1)
        return blocks

    shared = [("z", far_steps[0]), ("y", 0)] if direct else []

    def index_of(key):
        flip, o = "zy".index(key[0]), key[1]
        return lambda vocab, k: lax.rem(vocab // 2 + n_far - o, n_far) * 2 + lax.rem(vocab + flip, 2)

    every = [(axis, o) for axis in "zy" for o in steps] if direct else [0]
    indices = [index_of(key) for key in every] if direct else [lambda vocab, k: k]
    early = []

    def places_of(keys):
        return jnp.stack([index_of(key)(lax.axis_index("vocab"), 0) for key in keys]).astype(jnp.int32)

    payload = pack(residual, gain)
    evens = sorted(range(0, n_layer, 2), reverse=True)
    remote = {}
    own = gather(payload)
    for e in evens[:-1]:
        given = {key: over_layer(own[key], e) for key in shared}
        remote[e] = gather(over_layer(payload, e), given)

    chunks = chunks_of(columns)
    codes, stats = {d: [] for d in range(n_layer)}, {d: [] for d in range(n_layer)}
    after = payload
    for e in evens:
        mine = own if e == 0 else remote[e]
        theirs = {key: over_layer(x, 1) for key, x in mine.items()}

        def blocks_of(keys):
            return [[part[key] if part[key].ndim == 3 else part[key][None] for key in keys] for part in (mine, theirs)]

        parts, places = [None] * len(chunks), None
        if e and early:
            late = [key for key in every if key not in early]
            first_half, sums, _ = join(blocks_of(early), features, None, rows, after, None)
            for i, (first, count) in enumerate(chunks[:AHEAD]):
                parts[i] = part_call(weights, first_half, places_of(early), after, first, count)
                after = parts[i]
            joined = join(blocks_of(late), features, None, rows, after, sums)
            places = places_of(late)
        else:
            joined = join(blocks_of(every), features, indices, rows, after, None)
        for i, (first, count) in enumerate(chunks if e else [(0, columns)]):
            if places is not None and parts[i] is None:
                parts[i] = part_call(weights, first_half, places_of(early), after, first, count)
                after = parts[i]
            new_codes, new_stats = logits_call(
                weights, joined, places, parts[i] if e else None, after, rows, first, count
            )
            after = new_stats[0]
            for d in (e, e + 1):
                code = new_codes[d - e]
                codes[d].append(over_layer(code, d) if d else code)
                stats[d].append(new_stats[d - e])
    for d in range(n_layer):
        stat = stats[d][0] if len(stats[d]) == 1 else jnp.concatenate(stats[d])
        stats[d] = over_layer(stat, d) if d else stat

    distances = [0, 1] + [d for e in evens[:-1] for d in (e, e + 1)]
    total = combine([stats[d] for d in distances])
    if direct:
        total = combine([total, over_vocab(total, 0, 1)])
        totals = [total] + [over_vocab(total, o, 0) for o in far_steps]
    else:
        totals = [lax.all_gather(total, "vocab", tiled=True)]

    if columns % 8:
        lse = row_lse([jnp.concatenate(totals)])
        pieces = []
        for d in range(n_layer):
            code, parts = jnp.concatenate(codes[d]), []
            for at in range(0, columns, TILE):
                factor, shift = decode_terms(stats[d], at // TILE, lse)
                parts.append(jnp.log(code[at : at + TILE].astype(F32)) * factor + shift)
            pieces.append(jnp.concatenate(parts))
        order = lax.axis_index("layer") ^ jnp.arange(n_layer)
        return jnp.take(jnp.stack(pieces), order, axis=0).reshape(n_layer * columns, rows).T

    items_all = []
    for d in distances:
        first = 0
        for array in codes[d]:
            for at in range(0, array.shape[0], CHUNK):
                items_all.append((array, (min(CHUNK, array.shape[0] - at), first + at, d, distances.index(d), at)))
            first += array.shape[0]
    out = None
    for part in (items_all,):
        arrays, items = [], []
        for array, (count, first, d, source, at) in part:
            if not any(array is seen for seen in arrays):
                arrays.append(array)
            ref = [array is seen for seen in arrays].index(True)
            items.append((count, first, d, source, ref, at))
        out = write(arrays, items, [stats[d] for d in distances], totals, out, columns, n_layer * columns)
    return out.T


def solution(mesh):
    placed = (P("layer", "vocab"), P(None, "vocab"), P(None, ("vocab", "layer")))
    n_vocab, n_layer = mesh.shape["vocab"], mesh.shape["layer"]

    def body(residual, gain, unembed):
        return local(n_vocab, n_layer, residual, gain, unembed)

    mapped = jax.shard_map(body, mesh=mesh, in_specs=placed, out_specs=P("layer", "vocab"), check_vma=False)

    def step(residual, gain, unembed):
        return mapped(residual, gain, unembed)

    return step if n_vocab // 2 <= 4 else mapped
```
